32 devices in a mesh: section: 2 (over y), dp: 16 (over z, x, core).
Axes of the slice: x: 2, y: 2, z: 4, core: 2. Of those that a mesh axis runs over, the one named last changes fastest.
Arguments:
- inputs: bfloat16 [32, 128, 1536], P('dp'), parts along dimension 0, may hold values from -6 to 6
- w_query: bfloat16 [2, 1536, 768], P('section'), may hold values from -0.15625 to 0.15625
- w_key: bfloat16 [2, 1536, 768], P('section'), may hold values from -0.15625 to 0.15625
- w_value: bfloat16 [2, 1536, 768], P('section'), may hold values from -0.15625 to 0.15625
- w_out: bfloat16 [2, 768, 1536], P('section'), may hold values from -0.21875 to 0.21875
- mixing: float32 [2], P('section'), may hold values from 0.2 to 0.8
Outputs:
- outputs: bfloat16 [32, 128, 1536], P(('dp', 'section')), parts along dimension 0
The draws below stay inside these ranges and needn't reach their ends.
There are 16 independent parts, one for each index of `dp`. The reference program is written for one: setup_inputs(seed, part) draws one part's arguments, and reference() takes and returns one part's arrays. A program takes and returns all parts, laid end to end along the dimension named above; an argument that names none is the same for every part. Nothing has to cross between parts.
All inputs are finite; a program needn't handle non-finite values.
Results may differ from the reference program's by a relative error of at most 0.023.
Values may be sent and summed in bfloat16 or wider, within the bound.
A program may use at most 128 MiB of HBM per device.

```python
import jax
import jax.numpy as jnp
from jax import lax

D = 1536
HEADS = 6
HEAD_DIM = 128
SEQ = 128
HD = 768
MICRO = 2
LAYERS = 2


def level_of(stream_key, dims, split, low, top_value):
    def one(position, shards_of):
        draws = jax.random.uniform(jax.random.fold_in(jax.random.fold_in(stream_key, 6), position), (shards_of,), jnp.float32, low / len(split), top_value / len(split))
        return jnp.repeat(jnp.exp(draws), dims[position] // shards_of).reshape((-1,) + (1,) * (len(dims) - position - 1))

    gain = one(*split[0])
    for cut in split[1:]:
        gain = gain * one(*cut)
    return gain


def scatter_about(key, dims, width, reach, pieces=(), kind=jnp.bfloat16):
    entries = jax.random.normal(key, dims, jnp.float32) * width
    if len(pieces) > 0:
        entries = level_of(key, dims, pieces, -0.22, 0.18) * entries
    return jnp.clip(entries, min=-reach, max=reach).astype(kind)


def setup_inputs(seed: int = 0, part: int = 0) -> dict:
    key_of = jax.random.split(jax.random.key(seed), 7)
    part_keys = jax.random.split(jax.random.fold_in(key_of[6], part), 7)
    inputs = scatter_about(part_keys[0], (MICRO, SEQ, D), 1.0, 6.0)
    w_query = scatter_about(key_of[1], (LAYERS, D, HD), D ** -0.5, 0.15625, ((0, 2),))
    w_key = scatter_about(key_of[2], (LAYERS, D, HD), D ** -0.5, 0.15625, ((0, 2),))
    w_value = scatter_about(key_of[3], (LAYERS, D, HD), D ** -0.5, 0.15625, ((0, 2),))
    w_out = scatter_about(key_of[4], (LAYERS, HD, D), HD ** -0.5, 0.21875, ((0, 2),))
    mixing = jnp.clip(0.2 + 0.6 * jax.random.uniform(key_of[5], (LAYERS,), jnp.float32) ** level_of(key_of[5], (LAYERS,), ((0, 2),), -0.2, 0.2), 0.2, 0.8)
    return dict(inputs=inputs, w_query=w_query, w_key=w_key, w_value=w_value, w_out=w_out, mixing=mixing)


epsilon = 1e-06
score_scale = 0.12

def norm_rows(tensor):
    return tensor * lax.rsqrt(lax.optimization_barrier(jnp.mean(tensor * tensor, axis=-1, keepdims=True)) + epsilon)

def layer_apply(hidden, w_query, w_key, w_value, w_out, mixing, first_values, first_flag):
    row_count = hidden.shape[0]
    hidden_wide = hidden.astype(jnp.float32)
    normed = norm_rows(hidden_wide).astype(jnp.bfloat16)
    queries = jnp.dot(normed, w_query, preferred_element_type=jnp.float32).reshape(row_count, HEADS, HEAD_DIM)
    key_rows = jnp.dot(normed, w_key, preferred_element_type=jnp.float32).reshape(row_count, HEADS, HEAD_DIM)
    queries = norm_rows(queries).astype(jnp.bfloat16)
    key_rows = norm_rows(key_rows).astype(jnp.bfloat16)
    values = jnp.dot(normed, w_value, preferred_element_type=jnp.float32)
    own_values = values.astype(jnp.bfloat16)
    if first_flag:
        used_values = own_values
    else:
        used_values = (mixing * values + (1.0 - mixing) * first_values.astype(jnp.float32)).astype(jnp.bfloat16)
    used_values = used_values.reshape(row_count, HEADS, HEAD_DIM)
    scores = jnp.einsum('qhd,khd->hqk', queries.astype(jnp.float32), key_rows.astype(jnp.float32)) * score_scale
    positions = jnp.arange(row_count, dtype=jnp.int32)
    causal = positions[:, None] >= positions[None, :]
    weights = jnp.where(causal[None, :, :], jnp.exp(scores), 0.0)
    probabilities = (weights / lax.optimization_barrier(jnp.sum(weights, axis=-1, keepdims=True))).astype(jnp.bfloat16)
    attended = jnp.einsum('hqk,khd->qhd', probabilities.astype(jnp.float32), used_values.astype(jnp.float32))
    attended = attended.astype(jnp.bfloat16).reshape(row_count, HEADS * HEAD_DIM)
    result = (hidden_wide + jnp.dot(attended, w_out, preferred_element_type=jnp.float32)).astype(jnp.bfloat16)
    return (result, own_values)

def reference(inputs, w_query, w_key, w_value, w_out, mixing):
    finished = []
    for micro_index in range(inputs.shape[0]):
        hidden = inputs[micro_index]
        first_values = None
        for layer_number in range(w_query.shape[0]):
            hidden, own_values = layer_apply(hidden, w_query[layer_number], w_key[layer_number], w_value[layer_number], w_out[layer_number], mixing[layer_number], first_values, layer_number == 0)
            if layer_number == 0:
                first_values = own_values
        finished.append(hidden)
    return jnp.stack(finished)
```

```python
import functools

import jax
import jax.numpy as jnp
from jax import lax
from jax.experimental import pallas as pl
from jax.experimental.pallas import tpu as pltpu
from jax.sharding import PartitionSpec as P

HEADS = 6

epsilon = 1e-06
score_scale = 0.12
MESH = pl.DeviceIdType.MESH


def norm_rows(tensor):
    return tensor * lax.rsqrt(jnp.mean(tensor * tensor, axis=-1, keepdims=True) + epsilon)


def project(normed, weight):
    return jnp.dot(normed, weight, preferred_element_type=jnp.float32)


def kernel(
    sections,
    inputs_ref,
    wq_hbm,
    wk_hbm,
    wv_hbm,
    wo_hbm,
    mixing_ref,
    out_ref,
    wq,
    wk,
    wv,
    wo,
    h_in,
    h_out,
    v_buf,
    q_buf,
    k_buf,
    used_buf,
    att_buf,
    load_sem,
    hs_sem,
    hr_sem,
    vs_sem,
    vr_sem,
    os_sem,
    or_sem,
    local_sem,
):
    me = lax.axis_index("section")
    last = sections - 1
    micro, rows, width = h_in.shape
    features = v_buf.shape[2]
    head = features // HEADS
    share = micro // sections
    is_first = me == 0
    is_last = me == last

    input_loads = [
        pltpu.make_async_copy(inputs_ref.at[i], h_in.at[i], load_sem.at[4 + i]) for i in range(micro)
    ]
    loads = [
        pltpu.make_async_copy(source.at[0], target, load_sem.at[i])
        for i, (source, target) in enumerate(
            ((wv_hbm, wv), (wq_hbm, wq), (wk_hbm, wk), (wo_hbm, wo))
        )
    ]

    @pl.when(is_first)
    def _():
        input_loads[0].start()

    for load in loads:
        load.start()

    @pl.when(is_first)
    def _():
        for load in input_loads[1:]:
            load.start()

    barrier = pltpu.get_barrier_semaphore()
    for step in range(1, sections):
        pl.semaphore_signal(
            barrier,
            inc=1,
            device_id={"section": lax.rem(me + step, sections)},
            device_id_type=MESH,
        )
    pl.semaphore_wait(barrier, sections - 1)

    onward = jnp.minimum(me + 1, last)

    def h_copy(i):
        return pltpu.make_async_remote_copy(
            src_ref=h_out.at[i],
            dst_ref=h_in.at[i],
            send_sem=hs_sem.at[i],
            recv_sem=hr_sem.at[i],
            device_id={"section": onward},
            device_id_type=MESH,
        )

    def v_copy(i):
        return pltpu.make_async_remote_copy(
            src_ref=v_buf.at[i],
            dst_ref=v_buf.at[i],
            send_sem=vs_sem.at[i],
            recv_sem=vr_sem.at[i],
            device_id={"section": onward},
            device_id_type=MESH,
        )

    def out_copy(i):
        return pltpu.make_async_remote_copy(
            src_ref=h_out.at[i],
            dst_ref=out_ref.at[i % share],
            send_sem=os_sem.at[i],
            recv_sem=or_sem.at[i],
            device_id={"section": i // share},
            device_id_type=MESH,
        )

    def own_copy(i):
        return pltpu.make_async_copy(h_out.at[i], out_ref.at[i % share], local_sem.at[i])

    row_index = lax.broadcasted_iota(jnp.int32, (rows, rows), 0)
    column_index = lax.broadcasted_iota(jnp.int32, (rows, rows), 1)
    causal = row_index >= column_index

    def attend_and_out(i, normed):
        queries = project(normed, wq[...])
        for n in range(HEADS):
            part = slice(n * head, (n + 1) * head)
            q_buf[:, part] = norm_rows(queries[:, part]).astype(jnp.bfloat16)

        def keys_and_rest():
            key_rows = project(normed, wk[...])
            for n in range(HEADS):
                part = slice(n * head, (n + 1) * head)
                k_buf[:, part] = norm_rows(key_rows[:, part]).astype(jnp.bfloat16)
            for n in range(HEADS):
                part = slice(n * head, (n + 1) * head)
                scores = (
                    lax.dot_general(
                        q_buf[:, part],
                        k_buf[:, part],
                        (((1,), (1,)), ((), ())),
                        preferred_element_type=jnp.float32,
                    )
                    * score_scale
                )
                weights = jnp.where(causal, jnp.exp(scores), 0.0)
                probabilities = (weights / jnp.sum(weights, axis=-1, keepdims=True)).astype(
                    jnp.bfloat16
                )
                att_buf[:, part] = project(probabilities, used_buf[:, part]).astype(jnp.bfloat16)

        keys_and_rest()
        added = project(att_buf[...], wo[...])
        h_out[i] = (h_in[i].astype(jnp.float32) + added).astype(jnp.bfloat16)

    @pl.when(is_first)
    def _():
        for i in range(micro):
            input_loads[i].wait()
            normed = norm_rows(h_in[i].astype(jnp.float32)).astype(jnp.bfloat16)
            if i == 0:
                loads[0].wait()
            own = project(normed, wv[...]).astype(jnp.bfloat16)
            v_buf[i] = own
            used_buf[...] = own
            if sections > 1:
                v_copy(i).start()
            if i == 0:
                for load in loads[1:]:
                    load.wait()
            attend_and_out(i, normed)
            if sections > 1:
                h_copy(i).start()
            else:
                own_copy(i).start()

    if sections > 1:

        @pl.when(jnp.logical_not(is_first))
        def _():
            for load in loads:
                load.wait()
            mixing = mixing_ref[0]
            for i in range(micro):
                v_copy(i).wait_recv()
                if sections > 2:

                    @pl.when(jnp.logical_not(is_last))
                    def _():
                        v_copy(i).start()

                h_copy(i).wait_recv()
                normed = norm_rows(h_in[i].astype(jnp.float32)).astype(jnp.bfloat16)
                values = project(normed, wv[...])
                used_buf[...] = (
                    mixing * values + (1.0 - mixing) * v_buf[i].astype(jnp.float32)
                ).astype(jnp.bfloat16)
                attend_and_out(i, normed)

                @pl.when(is_last)
                def _():
                    if i // share == last:
                        own_copy(i).start()
                    else:
                        out_copy(i).start()

                if sections > 2:

                    @pl.when(jnp.logical_not(is_last))
                    def _():
                        h_copy(i).start()

    @pl.when(jnp.logical_not(is_last))
    def _():
        for i in range(micro):
            v_copy(i).wait_send()
            h_copy(i).wait_send()

    for i in range(micro):
        owner = i // share
        if owner == last:

            @pl.when(is_last)
            def _():
                own_copy(i).wait()

        else:

            @pl.when(is_last)
            def _():
                out_copy(i).wait_send()

            @pl.when(me == owner)
            def _():
                out_copy(i).wait_recv()


def body(inputs, w_query, w_key, w_value, w_out, mixing):
    sections = lax.axis_size("section")
    micro, rows, width = inputs.shape
    features = w_value.shape[2]
    share = micro // sections
    bf16 = jnp.bfloat16
    anywhere = pl.BlockSpec(memory_space=pl.ANY)
    dma = pltpu.SemaphoreType.DMA
    return pl.pallas_call(
        functools.partial(kernel, sections),
        out_shape=jax.ShapeDtypeStruct((share, rows, width), bf16),
        in_specs=[anywhere] * 5 + [pl.BlockSpec(memory_space=pltpu.SMEM)],
        out_specs=anywhere,
        scratch_shapes=[
            pltpu.VMEM((width, features), bf16),
            pltpu.VMEM((width, features), bf16),
            pltpu.VMEM((width, features), bf16),
            pltpu.VMEM((features, width), bf16),
            pltpu.VMEM((micro, rows, width), bf16),
            pltpu.VMEM((micro, rows, width), bf16),
            pltpu.VMEM((micro, rows, features), bf16),
            pltpu.VMEM((rows, features), bf16),
            pltpu.VMEM((rows, features), bf16),
            pltpu.VMEM((rows, features), bf16),
            pltpu.VMEM((rows, features), bf16),
            dma((4 + micro,)),
            dma((micro,)),
            dma((micro,)),
            dma((micro,)),
            dma((micro,)),
            dma((micro,)),
            dma((micro,)),
            dma((micro,)),
        ],
        compiler_params=pltpu.CompilerParams(
            collective_id=0, has_side_effects=True, vmem_limit_bytes=60 * 1024 * 1024
        ),
        name="sections",
    )(inputs, w_query, w_key, w_value, w_out, mixing)


def solution(mesh):
    in_specs = (
        P("dp", None, None),
        P("section", None, None),
        P("section", None, None),
        P("section", None, None),
        P("section", None, None),
        P("section"),
    )
    out_specs = P(("dp", "section"), None, None)
    return jax.shard_map(body, mesh=mesh, in_specs=in_specs, out_specs=out_specs, check_vma=False)
```

```python
import functools

import jax
import jax.numpy as jnp
from jax import lax
from jax.experimental import pallas as pl
from jax.experimental.pallas import tpu as pltpu
from jax.sharding import PartitionSpec as P

HEADS = 6

epsilon = 1e-06
score_scale = 0.12
MESH = pl.DeviceIdType.MESH


def norm_rows(tensor):
    return tensor * lax.rsqrt(jnp.mean(tensor * tensor, axis=-1, keepdims=True) + epsilon)


def project(normed, weight):
    return jnp.dot(normed, weight, preferred_element_type=jnp.float32)


def kernel(
    sections,
    inputs_ref,
    wq_hbm,
    wk_hbm,
    wv_hbm,
    wo_hbm,
    mixing_ref,
    out_ref,
    wq,
    wk,
    wv,
    wo,
    h_in,
    h_out,
    v_buf,
    q_buf,
    k_buf,
    val_buf,
    p_buf,
    att_buf,
    acc_buf,
    in_sem,
    wv_sem,
    load_sem,
    hs_sem,
    hr_sem,
    vs_sem,
    vr_sem,
    os_sem,
    or_sem,
):
    me = lax.axis_index("section")
    last = sections - 1
    micro, rows, width = h_in.shape
    features = v_buf.shape[2]
    head = features // HEADS
    chunks = HEADS // 2
    span = features // chunks
    share = micro // sections
    is_first = me == 0
    is_last = me == last
    bf16 = jnp.bfloat16
    f32 = jnp.float32

    def head_part(n):
        return slice(n * head, (n + 1) * head)

    def chunk_part(j):
        return slice(j * span, (j + 1) * span)

    def input_load(i):
        return pltpu.make_async_copy(inputs_ref.at[i], h_in.at[i], in_sem.at[i])

    def value_load(j):
        return pltpu.make_async_copy(
            wv_hbm.at[0, :, chunk_part(j)], wv.at[:, chunk_part(j)], wv_sem.at[j]
        )

    loads = [
        pltpu.make_async_copy(source.at[0], target, load_sem.at[i])
        for i, (source, target) in enumerate(((wq_hbm, wq), (wk_hbm, wk), (wo_hbm, wo)))
    ]

    barrier = pltpu.get_barrier_semaphore()
    for step in range(1, sections):
        pl.semaphore_signal(
            barrier,
            inc=1,
            device_id={"section": lax.rem(me + step, sections)},
            device_id_type=MESH,
        )

    @pl.when(is_first)
    def _():
        input_load(0).start()

    for j in range(chunks):
        value_load(j).start()
    for load in loads:
        load.start()

    @pl.when(is_first)
    def _():
        for i in range(1, micro):
            input_load(i).start()

    pl.semaphore_wait(barrier, sections - 1)

    onward = jnp.minimum(me + 1, last)

    def h_copy(i):
        return pltpu.make_async_remote_copy(
            src_ref=h_out.at[i],
            dst_ref=h_in.at[i],
            send_sem=hs_sem.at[i],
            recv_sem=hr_sem.at[i],
            device_id={"section": onward},
            device_id_type=MESH,
        )

    def v_copy(i, j):
        return pltpu.make_async_remote_copy(
            src_ref=v_buf.at[i, :, chunk_part(j)],
            dst_ref=v_buf.at[i, :, chunk_part(j)],
            send_sem=vs_sem.at[i, j],
            recv_sem=vr_sem.at[i, j],
            device_id={"section": onward},
            device_id_type=MESH,
        )

    def out_copy(i):
        return pltpu.make_async_remote_copy(
            src_ref=h_out.at[i],
            dst_ref=out_ref.at[i % share],
            send_sem=os_sem.at[i],
            recv_sem=or_sem.at[i],
            device_id={"section": i // share},
            device_id_type=MESH,
        )

    row_index = lax.broadcasted_iota(jnp.int32, (rows, rows), 0)
    column_index = lax.broadcasted_iota(jnp.int32, (rows, rows), 1)
    causal = row_index >= column_index

    def fill_probabilities(normed):
        queries = project(normed, wq[...])
        key_rows = project(normed, wk[...])
        for n in range(HEADS):
            q_buf[:, head_part(n)] = norm_rows(queries[:, head_part(n)]).astype(bf16)
            k_buf[:, head_part(n)] = norm_rows(key_rows[:, head_part(n)]).astype(bf16)
        for n in range(HEADS):
            scores = (
                lax.dot_general(
                    q_buf[:, head_part(n)],
                    k_buf[:, head_part(n)],
                    (((1,), (1,)), ((), ())),
                    preferred_element_type=f32,
                )
                * score_scale
            )
            weights = jnp.where(causal, jnp.exp(scores), 0.0)
            p_buf[n] = (weights / jnp.sum(weights, axis=-1, keepdims=True)).astype(bf16)

    @pl.when(is_first)
    def _():
        def one(i, carry):
            input_load(i).wait()
            normed = norm_rows(h_in[i].astype(f32)).astype(bf16)
            for j in range(chunks):

                @pl.when(i == 0)
                def _():
                    value_load(j).wait()

                v_buf[i, :, chunk_part(j)] = project(normed, wv[:, chunk_part(j)]).astype(bf16)
                if sections > 1:

                    @pl.when(i == 0)
                    def _():
                        v_copy(i, j).start()

            @pl.when(i == 0)
            def _():
                for load in loads:
                    load.wait()

            fill_probabilities(normed)
            for n in range(HEADS):
                att_buf[:, head_part(n)] = project(p_buf[n], v_buf[i, :, head_part(n)]).astype(bf16)
            result = (h_in[i].astype(f32) + project(att_buf[...], wo[...])).astype(bf16)
            if sections > 1:
                h_out[i] = result
                h_copy(i).start()

                @pl.when(i > 0)
                def _():
                    for j in range(chunks):
                        v_copy(i, j).start()

            else:
                out_ref[i] = result
            return carry

        lax.fori_loop(0, micro, one, 0)

    if sections > 1:

        @pl.when(jnp.logical_not(is_first))
        def _():
            for j in range(chunks):
                value_load(j).wait()
            for load in loads:
                load.wait()
            mixing = mixing_ref[0]

            def one(i, carry):
                h_copy(i).wait_recv()
                normed = norm_rows(h_in[i].astype(f32)).astype(bf16)
                fill_probabilities(normed)
                val_buf[...] = mixing * project(normed, wv[...])
                for j in range(chunks):
                    v_copy(i, j).wait_recv()
                    if sections > 2:

                        @pl.when(jnp.logical_not(is_last))
                        def _():
                            v_copy(i, j).start()

                    used = (
                        val_buf[:, chunk_part(j)]
                        + (1.0 - mixing) * v_buf[i, :, chunk_part(j)].astype(f32)
                    ).astype(bf16)
                    for n in range(2):
                        att_buf[:, head_part(2 * j + n)] = project(
                            p_buf[2 * j + n], used[:, head_part(n)]
                        ).astype(bf16)
                    term = project(att_buf[:, chunk_part(j)], wo[chunk_part(j), :])
                    if j == 0:
                        acc_buf[...] = term
                    elif j < chunks - 1:
                        acc_buf[...] += term
                result = (h_in[i].astype(f32) + (acc_buf[...] + term)).astype(bf16)
                mine = jnp.logical_and(is_last, i // share == last)

                @pl.when(mine)
                def _():
                    out_ref[i % share] = result

                @pl.when(jnp.logical_not(mine))
                def _():
                    h_out[i] = result

                    @pl.when(is_last)
                    def _():
                        out_copy(i).start()

                    if sections > 2:

                        @pl.when(jnp.logical_not(is_last))
                        def _():
                            h_copy(i).start()

                return carry

            lax.fori_loop(0, micro, one, 0)

    @pl.when(jnp.logical_not(is_last))
    def _():
        for i in range(micro):
            for j in range(chunks):
                v_copy(i, j).wait_send()
            h_copy(i).wait_send()

    for i in range(micro):
        if i // share != last:

            @pl.when(is_last)
            def _():
                out_copy(i).wait_send()

            @pl.when(me == i // share)
            def _():
                out_copy(i).wait_recv()


def body(inputs, w_query, w_key, w_value, w_out, mixing):
    sections = lax.axis_size("section")
    micro, rows, width = inputs.shape
    features = w_value.shape[2]
    share = micro // sections
    bf16 = jnp.bfloat16
    anywhere = pl.BlockSpec(memory_space=pltpu.HBM)
    dma = pltpu.SemaphoreType.DMA
    return pl.pallas_call(
        functools.partial(kernel, sections),
        out_shape=pltpu.VMEM((share, rows, width), bf16),
        in_specs=[anywhere] * 5 + [pl.BlockSpec(memory_space=pltpu.SMEM)],
        out_specs=pl.BlockSpec(memory_space=pltpu.VMEM),
        scratch_shapes=[
            pltpu.VMEM((width, features), bf16),
            pltpu.VMEM((width, features), bf16),
            pltpu.VMEM((width, features), bf16),
            pltpu.VMEM((features, width), bf16),
            pltpu.VMEM((micro, rows, width), bf16),
            pltpu.VMEM((micro, rows, width), bf16),
            pltpu.VMEM((micro, rows, features), bf16),
            pltpu.VMEM((rows, features), bf16),
            pltpu.VMEM((rows, features), bf16),
            pltpu.VMEM((rows, features), jnp.float32),
            pltpu.VMEM((HEADS, rows, rows), bf16),
            pltpu.VMEM((rows, features), bf16),
            pltpu.VMEM((rows, width), jnp.float32),
            dma((micro,)),
            dma((HEADS // 2,)),
            dma((3,)),
            dma((micro,)),
            dma((micro,)),
            dma((micro, HEADS // 2)),
            dma((micro, HEADS // 2)),
            dma((micro,)),
            dma((micro,)),
        ],
        compiler_params=pltpu.CompilerParams(
            collective_id=0, has_side_effects=True, vmem_limit_bytes=62 * 1024 * 1024
        ),
        name="sections",
    )(inputs, w_query, w_key, w_value, w_out, mixing)


def solution(mesh):
    in_specs = (
        P("dp", None, None),
        P("section", None, None),
        P("section", None, None),
        P("section", None, None),
        P("section", None, None),
        P("section"),
    )
    out_specs = P(("dp", "section"), None, None)
    return jax.shard_map(body, mesh=mesh, in_specs=in_specs, out_specs=out_specs, check_vma=False)
```

```python
import functools

import jax
import jax.numpy as jnp
from jax import lax
from jax.experimental import pallas as pl
from jax.experimental.pallas import tpu as pltpu
from jax.sharding import PartitionSpec as P

HEADS = 6

epsilon = 1e-06
score_scale = 0.12
MESH = pl.DeviceIdType.MESH


def norm_rows(tensor):
    return tensor * lax.rsqrt(jnp.mean(tensor * tensor, axis=-1, keepdims=True) + epsilon)


def project(normed, weight):
    return jnp.dot(normed, weight, preferred_element_type=jnp.float32)


def kernel(
    sections,
    inputs_ref,
    wq_hbm,
    wk_hbm,
    wv_hbm,
    wo_hbm,
    mixing_ref,
    out_ref,
    wq,
    wk,
    wv,
    wo,
    h_in,
    h_out,
    v_buf,
    q_buf,
    k_buf,
    val_buf,
    p_buf,
    att_buf,
    acc_buf,
    in_sem,
    wv_sem,
    load_sem,
    hs_sem,
    hr_sem,
    vs_sem,
    vr_sem,
    os_sem,
    or_sem,
):
    me = lax.axis_index("section")
    last = sections - 1
    micro, rows, width = h_in.shape
    features = v_buf.shape[2]
    head = features // HEADS
    chunks = HEADS // 2
    span = features // chunks
    share = micro // sections
    is_first = me == 0
    is_last = me == last
    bf16 = jnp.bfloat16
    f32 = jnp.float32

    def head_part(n):
        return slice(n * head, (n + 1) * head)

    def chunk_part(j):
        return slice(j * span, (j + 1) * span)

    def input_load(i):
        return pltpu.make_async_copy(inputs_ref.at[i], h_in.at[i], in_sem.at[i])

    def value_load(j):
        return pltpu.make_async_copy(
            wv_hbm.at[0, :, chunk_part(j)], wv.at[:, chunk_part(j)], wv_sem.at[j]
        )

    loads = [
        pltpu.make_async_copy(source.at[0], target, load_sem.at[i])
        for i, (source, target) in enumerate(((wq_hbm, wq), (wk_hbm, wk), (wo_hbm, wo)))
    ]

    barrier = pltpu.get_barrier_semaphore()
    for step in range(1, sections):
        pl.semaphore_signal(
            barrier,
            inc=1,
            device_id={"section": lax.rem(me + step, sections)},
            device_id_type=MESH,
        )

    @pl.when(is_first)
    def _():
        input_load(0).start()
        value_load(0).start()

    if sections > 1:

        @pl.when(jnp.logical_not(is_first))
        def _():
            for j in range(chunks):
                value_load(j).start()
            for load in loads:
                load.start()

    pl.semaphore_wait(barrier, sections - 1)

    onward = jnp.minimum(me + 1, last)

    def h_copy(i):
        return pltpu.make_async_remote_copy(
            src_ref=h_out.at[i],
            dst_ref=h_in.at[i],
            send_sem=hs_sem.at[i],
            recv_sem=hr_sem.at[i],
            device_id={"section": onward},
            device_id_type=MESH,
        )

    def v_copy(i, j):
        return pltpu.make_async_remote_copy(
            src_ref=v_buf.at[i, :, chunk_part(j)],
            dst_ref=v_buf.at[i, :, chunk_part(j)],
            send_sem=vs_sem.at[i, j],
            recv_sem=vr_sem.at[i, j],
            device_id={"section": onward},
            device_id_type=MESH,
        )

    def out_copy(i):
        return pltpu.make_async_remote_copy(
            src_ref=h_out.at[i],
            dst_ref=out_ref.at[i % share],
            send_sem=os_sem.at[i],
            recv_sem=or_sem.at[i],
            device_id={"section": i // share},
            device_id_type=MESH,
        )

    row_index = lax.broadcasted_iota(jnp.int32, (rows, rows), 0)
    column_index = lax.broadcasted_iota(jnp.int32, (rows, rows), 1)
    causal = row_index >= column_index

    def fill_probabilities(normed):
        queries = project(normed, wq[...])
        key_rows = project(normed, wk[...])
        for n in range(HEADS):
            q_buf[:, head_part(n)] = norm_rows(queries[:, head_part(n)]).astype(bf16)
            k_buf[:, head_part(n)] = norm_rows(key_rows[:, head_part(n)]).astype(bf16)
        for n in range(HEADS):
            scores = (
                lax.dot_general(
                    q_buf[:, head_part(n)],
                    k_buf[:, head_part(n)],
                    (((1,), (1,)), ((), ())),
                    preferred_element_type=f32,
                )
                * score_scale
            )
            weights = jnp.where(causal, jnp.exp(scores), 0.0)
            p_buf[n] = (weights / jnp.sum(weights, axis=-1, keepdims=True)).astype(bf16)

    @pl.when(is_first)
    def _():
        def one(i, carry):
            input_load(i).wait()

            @pl.when(i == 0)
            def _():
                for j in range(1, chunks):
                    value_load(j).start()

            normed = norm_rows(h_in[i].astype(f32)).astype(bf16)
            for j in range(chunks):

                @pl.when(i == 0)
                def _():
                    value_load(j).wait()
                    if j == 0:
                        for load in loads:
                            load.start()
                        for later in range(1, micro):
                            input_load(later).start()

                v_buf[i, :, chunk_part(j)] = project(normed, wv[:, chunk_part(j)]).astype(bf16)
                if sections > 1:

                    @pl.when(i == 0)
                    def _():
                        v_copy(i, j).start()

            @pl.when(i == 0)
            def _():
                for load in loads:
                    load.wait()

            fill_probabilities(normed)
            for n in range(HEADS):
                att_buf[:, head_part(n)] = project(p_buf[n], v_buf[i, :, head_part(n)]).astype(bf16)
            result = (h_in[i].astype(f32) + project(att_buf[...], wo[...])).astype(bf16)
            if sections > 1:
                h_out[i] = result
                h_copy(i).start()

                @pl.when(i > 0)
                def _():
                    for j in range(chunks):
                        v_copy(i, j).start()

            else:
                out_ref[i] = result
            return carry

        lax.fori_loop(0, micro, one, 0)

    if sections > 1:

        @pl.when(jnp.logical_not(is_first))
        def _():
            for j in range(chunks):
                value_load(j).wait()
            for load in loads:
                load.wait()
            mixing = mixing_ref[0]

            def one(i, carry):
                h_copy(i).wait_recv()
                normed = norm_rows(h_in[i].astype(f32)).astype(bf16)
                fill_probabilities(normed)
                val_buf[...] = mixing * project(normed, wv[...])
                for j in range(chunks):
                    v_copy(i, j).wait_recv()
                    if sections > 2:

                        @pl.when(jnp.logical_not(is_last))
                        def _():
                            v_copy(i, j).start()

                    used = (
                        val_buf[:, chunk_part(j)]
                        + (1.0 - mixing) * v_buf[i, :, chunk_part(j)].astype(f32)
                    ).astype(bf16)
                    for n in range(2):
                        att_buf[:, head_part(2 * j + n)] = project(
                            p_buf[2 * j + n], used[:, head_part(n)]
                        ).astype(bf16)
                    term = project(att_buf[:, chunk_part(j)], wo[chunk_part(j), :])
                    if j == 0:
                        acc_buf[...] = term
                    elif j < chunks - 1:
                        acc_buf[...] += term
                result = (h_in[i].astype(f32) + (acc_buf[...] + term)).astype(bf16)
                mine = jnp.logical_and(is_last, i // share == last)

                @pl.when(mine)
                def _():
                    out_ref[i % share] = result

                @pl.when(jnp.logical_not(mine))
                def _():
                    h_out[i] = result

                    @pl.when(is_last)
                    def _():
                        out_copy(i).start()

                    if sections > 2:

                        @pl.when(jnp.logical_not(is_last))
                        def _():
                            h_copy(i).start()

                return carry

            lax.fori_loop(0, micro, one, 0)

    @pl.when(jnp.logical_not(is_last))
    def _():
        for i in range(micro):
            for j in range(chunks):
                v_copy(i, j).wait_send()
            h_copy(i).wait_send()

    for i in range(micro):
        if i // share != last:

            @pl.when(is_last)
            def _():
                out_copy(i).wait_send()

            @pl.when(me == i // share)
            def _():
                out_copy(i).wait_recv()


def body(inputs, w_query, w_key, w_value, w_out, mixing):
    sections = lax.axis_size("section")
    micro, rows, width = inputs.shape
    features = w_value.shape[2]
    share = micro // sections
    bf16 = jnp.bfloat16
    anywhere = pl.BlockSpec(memory_space=pltpu.HBM)
    dma = pltpu.SemaphoreType.DMA
    return pl.pallas_call(
        functools.partial(kernel, sections),
        out_shape=pltpu.VMEM((share, rows, width), bf16),
        in_specs=[anywhere] * 5 + [pl.BlockSpec(memory_space=pltpu.SMEM)],
        out_specs=pl.BlockSpec(memory_space=pltpu.VMEM),
        scratch_shapes=[
            pltpu.VMEM((width, features), bf16),
            pltpu.VMEM((width, features), bf16),
            pltpu.VMEM((width, features), bf16),
            pltpu.VMEM((features, width), bf16),
            pltpu.VMEM((micro, rows, width), bf16),
            pltpu.VMEM((micro, rows, width), bf16),
            pltpu.VMEM((micro, rows, features), bf16),
            pltpu.VMEM((rows, features), bf16),
            pltpu.VMEM((rows, features), bf16),
            pltpu.VMEM((rows, features), jnp.float32),
            pltpu.VMEM((HEADS, rows, rows), bf16),
            pltpu.VMEM((rows, features), bf16),
            pltpu.VMEM((rows, width), jnp.float32),
            dma((micro,)),
            dma((HEADS // 2,)),
            dma((3,)),
            dma((micro,)),
            dma((micro,)),
            dma((micro, HEADS // 2)),
            dma((micro, HEADS // 2)),
            dma((micro,)),
            dma((micro,)),
        ],
        compiler_params=pltpu.CompilerParams(
            collective_id=0, has_side_effects=True, vmem_limit_bytes=62 * 1024 * 1024
        ),
        name="sections",
    )(inputs, w_query, w_key, w_value, w_out, mixing)


def solution(mesh):
    in_specs = (
        P("dp", None, None),
        P("section", None, None),
        P("section", None, None),
        P("section", None, None),
        P("section", None, None),
        P("section"),
    )
    out_specs = P(("dp", "section"), None, None)
    return jax.shard_map(body, mesh=mesh, in_specs=in_specs, out_specs=out_specs, check_vma=False)
```

```python
import functools

import jax
import jax.numpy as jnp
from jax import lax
from jax.experimental import pallas as pl
from jax.experimental.pallas import tpu as pltpu
from jax.sharding import PartitionSpec as P

HEADS = 6

epsilon = 1e-06
score_scale = 0.12
MESH = pl.DeviceIdType.MESH


def norm_rows(tensor):
    return tensor * lax.rsqrt(jnp.mean(tensor * tensor, axis=-1, keepdims=True) + epsilon)


def project(normed, weight):
    return jnp.dot(normed, weight, preferred_element_type=jnp.float32)


def kernel(
    sections,
    inputs_ref,
    wq_hbm,
    wk_hbm,
    wv_hbm,
    wo_hbm,
    mixing_ref,
    out_ref,
    wq,
    wk,
    wv,
    wo,
    h_in,
    h_out,
    v_buf,
    q_buf,
    k_buf,
    val_buf,
    p_buf,
    att_buf,
    acc_buf,
    in_sem,
    wv_sem,
    load_sem,
    hs_sem,
    hr_sem,
    vs_sem,
    vr_sem,
    os_sem,
    or_sem,
):
    me = lax.axis_index("section")
    last = sections - 1
    micro, rows, width = h_in.shape
    features = v_buf.shape[2]
    head = features // HEADS
    chunks = HEADS // 2
    span = features // chunks
    share = micro // sections
    is_first = me == 0
    is_last = me == last
    bf16 = jnp.bfloat16
    f32 = jnp.float32

    def head_part(n):
        return slice(n * head, (n + 1) * head)

    def chunk_part(j):
        return slice(j * span, (j + 1) * span)

    def column_part(c):
        return slice(c * (width // chunks), (c + 1) * (width // chunks))

    def input_load(i):
        return pltpu.make_async_copy(inputs_ref.at[i], h_in.at[i], in_sem.at[i])

    def value_load(j):
        return pltpu.make_async_copy(
            wv_hbm.at[0, :, chunk_part(j)], wv.at[:, chunk_part(j)], wv_sem.at[j]
        )

    loads = [
        pltpu.make_async_copy(source.at[0], target, load_sem.at[i])
        for i, (source, target) in enumerate(((wq_hbm, wq), (wk_hbm, wk), (wo_hbm, wo)))
    ]

    barrier = pltpu.get_barrier_semaphore()
    for step in range(1, sections):
        pl.semaphore_signal(
            barrier,
            inc=1,
            device_id={"section": lax.rem(me + step, sections)},
            device_id_type=MESH,
        )

    @pl.when(is_first)
    def _():
        input_load(0).start()

    for j in range(chunks):
        value_load(j).start()
    for load in loads:
        load.start()

    @pl.when(is_first)
    def _():
        for i in range(1, micro):
            input_load(i).start()

    pl.semaphore_wait(barrier, sections - 1)

    onward = jnp.minimum(me + 1, last)

    def h_copy(i, c):
        return pltpu.make_async_remote_copy(
            src_ref=h_out.at[i, :, column_part(c)],
            dst_ref=h_in.at[i, :, column_part(c)],
            send_sem=hs_sem.at[i, c],
            recv_sem=hr_sem.at[i, c],
            device_id={"section": onward},
            device_id_type=MESH,
        )

    def v_copy(i, j):
        return pltpu.make_async_remote_copy(
            src_ref=v_buf.at[i, :, chunk_part(j)],
            dst_ref=v_buf.at[i, :, chunk_part(j)],
            send_sem=vs_sem.at[i, j],
            recv_sem=vr_sem.at[i, j],
            device_id={"section": onward},
            device_id_type=MESH,
        )

    def out_copy(i, c):
        return pltpu.make_async_remote_copy(
            src_ref=h_out.at[i, :, column_part(c)],
            dst_ref=out_ref.at[i % share, :, column_part(c)],
            send_sem=os_sem.at[i, c],
            recv_sem=or_sem.at[i, c],
            device_id={"section": i // share},
            device_id_type=MESH,
        )

    row_index = lax.broadcasted_iota(jnp.int32, (rows, rows), 0)
    column_index = lax.broadcasted_iota(jnp.int32, (rows, rows), 1)
    causal = row_index >= column_index

    def fill_probabilities(normed):
        queries = project(normed, wq[...])
        key_rows = project(normed, wk[...])
        for n in range(HEADS):
            q_buf[:, head_part(n)] = norm_rows(queries[:, head_part(n)]).astype(bf16)
            k_buf[:, head_part(n)] = norm_rows(key_rows[:, head_part(n)]).astype(bf16)
        for n in range(HEADS):
            scores = (
                lax.dot_general(
                    q_buf[:, head_part(n)],
                    k_buf[:, head_part(n)],
                    (((1,), (1,)), ((), ())),
                    preferred_element_type=f32,
                )
                * score_scale
            )
            weights = jnp.where(causal, jnp.exp(scores), 0.0)
            p_buf[n] = (weights / jnp.sum(weights, axis=-1, keepdims=True)).astype(bf16)

    @pl.when(is_first)
    def _():
        def one(i, carry):
            input_load(i).wait()
            normed = norm_rows(h_in[i].astype(f32)).astype(bf16)
            for j in range(chunks):

                @pl.when(i == 0)
                def _():
                    value_load(j).wait()

                v_buf[i, :, chunk_part(j)] = project(normed, wv[:, chunk_part(j)]).astype(bf16)
                if sections > 1:

                    @pl.when(i == 0)
                    def _():
                        v_copy(i, j).start()

            @pl.when(i == 0)
            def _():
                for load in loads:
                    load.wait()

            fill_probabilities(normed)
            for n in range(HEADS):
                att_buf[:, head_part(n)] = project(p_buf[n], v_buf[i, :, head_part(n)]).astype(bf16)
            for c in range(chunks):
                part = column_part(c)
                added = project(att_buf[...], wo[:, part])
                result = (h_in[i, :, part].astype(f32) + added).astype(bf16)
                if sections > 1:
                    h_out[i, :, part] = result
                    h_copy(i, c).start()
                else:
                    out_ref[i, :, part] = result
            if sections > 1:

                @pl.when(i > 0)
                def _():
                    for j in range(chunks):
                        v_copy(i, j).start()

            return carry

        lax.fori_loop(0, micro, one, 0)

    if sections > 1:

        @pl.when(jnp.logical_not(is_first))
        def _():
            for j in range(chunks):
                value_load(j).wait()
            for load in loads:
                load.wait()
            mixing = mixing_ref[0]

            def one(i, carry):
                for c in range(chunks):
                    h_copy(i, c).wait_recv()
                normed = norm_rows(h_in[i].astype(f32)).astype(bf16)
                fill_probabilities(normed)
                val_buf[...] = mixing * project(normed, wv[...])
                for j in range(chunks):
                    v_copy(i, j).wait_recv()
                    if sections > 2:

                        @pl.when(jnp.logical_not(is_last))
                        def _():
                            v_copy(i, j).start()

                    used = (
                        val_buf[:, chunk_part(j)]
                        + (1.0 - mixing) * v_buf[i, :, chunk_part(j)].astype(f32)
                    ).astype(bf16)
                    for n in range(2):
                        att_buf[:, head_part(2 * j + n)] = project(
                            p_buf[2 * j + n], used[:, head_part(n)]
                        ).astype(bf16)
                    if j < chunks - 1:
                        term = project(att_buf[:, chunk_part(j)], wo[chunk_part(j), :])
                        if j == 0:
                            acc_buf[...] = term
                        else:
                            acc_buf[...] += term
                mine = jnp.logical_and(is_last, i // share == last)
                for c in range(chunks):
                    part = column_part(c)
                    term = project(att_buf[:, chunk_part(chunks - 1)], wo[chunk_part(chunks - 1), part])
                    result = (h_in[i, :, part].astype(f32) + (acc_buf[:, part] + term)).astype(bf16)

                    @pl.when(mine)
                    def _():
                        out_ref[i % share, :, part] = result

                    @pl.when(jnp.logical_not(mine))
                    def _():
                        h_out[i, :, part] = result

                        @pl.when(is_last)
                        def _():
                            out_copy(i, c).start()

                        if sections > 2:

                            @pl.when(jnp.logical_not(is_last))
                            def _():
                                h_copy(i, c).start()

                return carry

            lax.fori_loop(0, micro, one, 0)

    @pl.when(jnp.logical_not(is_last))
    def _():
        for i in range(micro):
            for j in range(chunks):
                v_copy(i, j).wait_send()
                h_copy(i, j).wait_send()

    for i in range(micro):
        if i // share != last:

            @pl.when(is_last)
            def _():
                for c in range(chunks):
                    out_copy(i, c).wait_send()

            @pl.when(me == i // share)
            def _():
                for c in range(chunks):
                    out_copy(i, c).wait_recv()


def body(inputs, w_query, w_key, w_value, w_out, mixing):
    sections = lax.axis_size("section")
    micro, rows, width = inputs.shape
    features = w_value.shape[2]
    share = micro // sections
    bf16 = jnp.bfloat16
    anywhere = pl.BlockSpec(memory_space=pltpu.HBM)
    dma = pltpu.SemaphoreType.DMA
    return pl.pallas_call(
        functools.partial(kernel, sections),
        out_shape=pltpu.VMEM((share, rows, width), bf16),
        in_specs=[anywhere] * 5 + [pl.BlockSpec(memory_space=pltpu.SMEM)],
        out_specs=pl.BlockSpec(memory_space=pltpu.VMEM),
        scratch_shapes=[
            pltpu.VMEM((width, features), bf16),
            pltpu.VMEM((width, features), bf16),
            pltpu.VMEM((width, features), bf16),
            pltpu.VMEM((features, width), bf16),
            pltpu.VMEM((micro, rows, width), bf16),
            pltpu.VMEM((micro, rows, width), bf16),
            pltpu.VMEM((micro, rows, features), bf16),
            pltpu.VMEM((rows, features), bf16),
            pltpu.VMEM((rows, features), bf16),
            pltpu.VMEM((rows, features), jnp.float32),
            pltpu.VMEM((HEADS, rows, rows), bf16),
            pltpu.VMEM((rows, features), bf16),
            pltpu.VMEM((rows, width), jnp.float32),
            dma((micro,)),
            dma((HEADS // 2,)),
            dma((3,)),
            dma((micro, HEADS // 2)),
            dma((micro, HEADS // 2)),
            dma((micro, HEADS // 2)),
            dma((micro, HEADS // 2)),
            dma((micro, HEADS // 2)),
            dma((micro, HEADS // 2)),
        ],
        compiler_params=pltpu.CompilerParams(
            collective_id=0, has_side_effects=True, vmem_limit_bytes=62 * 1024 * 1024
        ),
        name="sections",
    )(inputs, w_query, w_key, w_value, w_out, mixing)


def solution(mesh):
    in_specs = (
        P("dp", None, None),
        P("section", None, None),
        P("section", None, None),
        P("section", None, None),
        P("section", None, None),
        P("section"),
    )
    out_specs = P(("dp", "section"), None, None)
    return jax.shard_map(body, mesh=mesh, in_specs=in_specs, out_specs=out_specs, check_vma=False)
```

```python
import functools

import jax
import jax.numpy as jnp
from jax import lax
from jax.experimental import pallas as pl
from jax.experimental.pallas import tpu as pltpu
from jax.sharding import PartitionSpec as P

HEADS = 6

epsilon = 1e-06
score_scale = 0.12
MESH = pl.DeviceIdType.MESH


def norm_rows(tensor):
    return tensor * lax.rsqrt(jnp.mean(tensor * tensor, axis=-1, keepdims=True) + epsilon)


def project(normed, weight):
    return jnp.dot(normed, weight, preferred_element_type=jnp.float32)


def kernel(
    sections,
    inputs_ref,
    wq_hbm,
    wk_hbm,
    wv_hbm,
    wo_hbm,
    mixing_ref,
    out_ref,
    wq,
    wk,
    wv,
    wo,
    h_in,
    h_out,
    v_buf,
    q_buf,
    k_buf,
    val_buf,
    p_buf,
    att_buf,
    acc_buf,
    in_sem,
    wv_sem,
    load_sem,
    hs_sem,
    hr_sem,
    vs_sem,
    vr_sem,
    os_sem,
    or_sem,
):
    me = lax.axis_index("section")
    last = sections - 1
    micro, rows, width = h_in.shape
    features = v_buf.shape[2]
    head = features // HEADS
    chunks = HEADS // 2
    span = features // chunks
    share = micro // sections
    is_first = me == 0
    is_last = me == last
    bf16 = jnp.bfloat16
    f32 = jnp.float32

    def head_part(n):
        return slice(n * head, (n + 1) * head)

    def chunk_part(j):
        return slice(j * span, (j + 1) * span)

    def input_load(i):
        return pltpu.make_async_copy(inputs_ref.at[i], h_in.at[i], in_sem.at[i])

    def value_load(j):
        return pltpu.make_async_copy(
            wv_hbm.at[0, :, chunk_part(j)], wv.at[:, chunk_part(j)], wv_sem.at[j]
        )

    loads = [
        pltpu.make_async_copy(source.at[0], target, load_sem.at[i])
        for i, (source, target) in enumerate(((wq_hbm, wq), (wk_hbm, wk), (wo_hbm, wo)))
    ]

    barrier = pltpu.get_barrier_semaphore()
    for step in range(1, sections):
        pl.semaphore_signal(
            barrier,
            inc=1,
            device_id={"section": lax.rem(me + step, sections)},
            device_id_type=MESH,
        )

    @pl.when(is_first)
    def _():
        input_load(0).start()

    for j in range(chunks):
        value_load(j).start()
    for load in loads:
        load.start()

    @pl.when(is_first)
    def _():
        for i in range(1, micro):
            input_load(i).start()

    pl.semaphore_wait(barrier, sections - 1)

    onward = jnp.minimum(me + 1, last)

    def h_copy(i):
        return pltpu.make_async_remote_copy(
            src_ref=h_out.at[i],
            dst_ref=h_in.at[i],
            send_sem=hs_sem.at[i],
            recv_sem=hr_sem.at[i],
            device_id={"section": onward},
            device_id_type=MESH,
        )

    def v_copy(i, j):
        return pltpu.make_async_remote_copy(
            src_ref=v_buf.at[i, :, chunk_part(j)],
            dst_ref=v_buf.at[i, :, chunk_part(j)],
            send_sem=vs_sem.at[i, j],
            recv_sem=vr_sem.at[i, j],
            device_id={"section": onward},
            device_id_type=MESH,
        )

    def out_copy(i):
        return pltpu.make_async_remote_copy(
            src_ref=h_out.at[i],
            dst_ref=out_ref.at[i % share],
            send_sem=os_sem.at[i],
            recv_sem=or_sem.at[i],
            device_id={"section": i // share},
            device_id_type=MESH,
        )

    row_index = lax.broadcasted_iota(jnp.int32, (rows, rows), 0)
    column_index = lax.broadcasted_iota(jnp.int32, (rows, rows), 1)
    causal = row_index >= column_index

    def fill_probabilities(normed, arrived):
        arrived(0)
        queries = project(normed, wq[...])
        for n in range(HEADS):
            q_buf[:, head_part(n)] = norm_rows(queries[:, head_part(n)]).astype(bf16)
        arrived(1)
        key_rows = project(normed, wk[...])
        for n in range(HEADS):
            k_buf[:, head_part(n)] = norm_rows(key_rows[:, head_part(n)]).astype(bf16)
        for n in range(HEADS):
            scores = (
                lax.dot_general(
                    q_buf[:, head_part(n)],
                    k_buf[:, head_part(n)],
                    (((1,), (1,)), ((), ())),
                    preferred_element_type=f32,
                )
                * score_scale
            )
            weights = jnp.where(causal, jnp.exp(scores), 0.0)
            p_buf[n] = (weights / jnp.sum(weights, axis=-1, keepdims=True)).astype(bf16)

    @pl.when(is_first)
    def _():
        def one(i, carry):
            input_load(i).wait()
            normed = norm_rows(h_in[i].astype(f32)).astype(bf16)
            for j in range(chunks):

                @pl.when(i == 0)
                def _():
                    value_load(j).wait()

                v_buf[i, :, chunk_part(j)] = project(normed, wv[:, chunk_part(j)]).astype(bf16)
                if sections > 1:

                    @pl.when(i == 0)
                    def _():
                        v_copy(i, j).start()

            def arrived(which):
                @pl.when(i == 0)
                def _():
                    loads[which].wait()

            fill_probabilities(normed, arrived)
            for n in range(HEADS):
                att_buf[:, head_part(n)] = project(p_buf[n], v_buf[i, :, head_part(n)]).astype(bf16)
            arrived(2)
            result = (h_in[i].astype(f32) + project(att_buf[...], wo[...])).astype(bf16)
            if sections > 1:
                h_out[i] = result
                h_copy(i).start()

                @pl.when(i > 0)
                def _():
                    for j in range(chunks):
                        v_copy(i, j).start()

            else:
                out_ref[i] = result
            return carry

        lax.fori_loop(0, micro, one, 0)

    if sections > 1:

        @pl.when(jnp.logical_not(is_first))
        def _():
            for j in range(chunks):
                value_load(j).wait()
            for load in loads:
                load.wait()
            mixing = mixing_ref[0]

            def one(i, carry):
                h_copy(i).wait_recv()
                normed = norm_rows(h_in[i].astype(f32)).astype(bf16)
                fill_probabilities(normed, lambda which: None)
                val_buf[...] = mixing * project(normed, wv[...])
                for j in range(chunks):
                    v_copy(i, j).wait_recv()
                    if sections > 2:

                        @pl.when(jnp.logical_not(is_last))
                        def _():
                            v_copy(i, j).start()

                    used = (
                        val_buf[:, chunk_part(j)]
                        + (1.0 - mixing) * v_buf[i, :, chunk_part(j)].astype(f32)
                    ).astype(bf16)
                    for n in range(2):
                        att_buf[:, head_part(2 * j + n)] = project(
                            p_buf[2 * j + n], used[:, head_part(n)]
                        ).astype(bf16)
                    term = project(att_buf[:, chunk_part(j)], wo[chunk_part(j), :])
                    if j == 0:
                        acc_buf[...] = term
                    elif j < chunks - 1:
                        acc_buf[...] += term
                result = (h_in[i].astype(f32) + (acc_buf[...] + term)).astype(bf16)
                mine = jnp.logical_and(is_last, i // share == last)

                @pl.when(mine)
                def _():
                    out_ref[i % share] = result

                @pl.when(jnp.logical_not(mine))
                def _():
                    h_out[i] = result

                    @pl.when(is_last)
                    def _():
                        out_copy(i).start()

                    if sections > 2:

                        @pl.when(jnp.logical_not(is_last))
                        def _():
                            h_copy(i).start()

                return carry

            lax.fori_loop(0, micro, one, 0)

    @pl.when(jnp.logical_not(is_last))
    def _():
        for i in range(micro):
            for j in range(chunks):
                v_copy(i, j).wait_send()
            h_copy(i).wait_send()

    for i in range(micro):
        if i // share != last:

            @pl.when(is_last)
            def _():
                out_copy(i).wait_send()

            @pl.when(me == i // share)
            def _():
                out_copy(i).wait_recv()


def body(inputs, w_query, w_key, w_value, w_out, mixing):
    sections = lax.axis_size("section")
    micro, rows, width = inputs.shape
    features = w_value.shape[2]
    share = micro // sections
    bf16 = jnp.bfloat16
    anywhere = pl.BlockSpec(memory_space=pltpu.HBM)
    dma = pltpu.SemaphoreType.DMA
    return pl.pallas_call(
        functools.partial(kernel, sections),
        out_shape=pltpu.VMEM((share, rows, width), bf16),
        in_specs=[anywhere] * 5 + [pl.BlockSpec(memory_space=pltpu.SMEM)],
        out_specs=pl.BlockSpec(memory_space=pltpu.VMEM),
        scratch_shapes=[
            pltpu.VMEM((width, features), bf16),
            pltpu.VMEM((width, features), bf16),
            pltpu.VMEM((width, features), bf16),
            pltpu.VMEM((features, width), bf16),
            pltpu.VMEM((micro, rows, width), bf16),
            pltpu.VMEM((micro, rows, width), bf16),
            pltpu.VMEM((micro, rows, features), bf16),
            pltpu.VMEM((rows, features), bf16),
            pltpu.VMEM((rows, features), bf16),
            pltpu.VMEM((rows, features), jnp.float32),
            pltpu.VMEM((HEADS, rows, rows), bf16),
            pltpu.VMEM((rows, features), bf16),
            pltpu.VMEM((rows, width), jnp.float32),
            dma((micro,)),
            dma((HEADS // 2,)),
            dma((3,)),
            dma((micro,)),
            dma((micro,)),
            dma((micro, HEADS // 2)),
            dma((micro, HEADS // 2)),
            dma((micro,)),
            dma((micro,)),
        ],
        compiler_params=pltpu.CompilerParams(
            collective_id=0, has_side_effects=True, vmem_limit_bytes=62 * 1024 * 1024
        ),
        name="sections",
    )(inputs, w_query, w_key, w_value, w_out, mixing)


def solution(mesh):
    in_specs = (
        P("dp", None, None),
        P("section", None, None),
        P("section", None, None),
        P("section", None, None),
        P("section", None, None),
        P("section"),
    )
    out_specs = P(("dp", "section"), None, None)
    return jax.shard_map(body, mesh=mesh, in_specs=in_specs, out_specs=out_specs, check_vma=False)
```

```python
import functools

import jax
import jax.numpy as jnp
from jax import lax
from jax.experimental import pallas as pl
from jax.experimental.pallas import tpu as pltpu
from jax.sharding import PartitionSpec as P

HEADS = 6

epsilon = 1e-06
score_scale = 0.12
MESH = pl.DeviceIdType.MESH


def norm_rows(tensor):
    return tensor * lax.rsqrt(jnp.mean(tensor * tensor, axis=-1, keepdims=True) + epsilon)


def project(normed, weight):
    return jnp.dot(normed, weight, preferred_element_type=jnp.float32)


def kernel(
    sections,
    inputs_ref,
    wq_hbm,
    wk_hbm,
    wv_hbm,
    wo_hbm,
    mixing_ref,
    out_ref,
    wq,
    wk,
    wv,
    wo,
    h_in,
    h_out,
    v_buf,
    q_buf,
    k_buf,
    val_buf,
    p_buf,
    att_buf,
    acc_buf,
    in_sem,
    wv_sem,
    load_sem,
    hs_sem,
    hr_sem,
    vs_sem,
    vr_sem,
    os_sem,
    or_sem,
):
    me = lax.axis_index("section")
    last = sections - 1
    micro, rows, width = h_in.shape
    features = v_buf.shape[2]
    head = features // HEADS
    chunks = HEADS // 2
    span = features // chunks
    share = micro // sections
    is_first = me == 0
    is_last = me == last
    bf16 = jnp.bfloat16
    f32 = jnp.float32

    def over_sequences(one):
        if micro > 2:
            lax.fori_loop(0, micro, one, 0)
        else:
            for i in range(micro):
                one(i, 0)

    def head_part(n):
        return slice(n * head, (n + 1) * head)

    def chunk_part(j):
        return slice(j * span, (j + 1) * span)

    def input_load(i):
        return pltpu.make_async_copy(inputs_ref.at[i], h_in.at[i], in_sem.at[i])

    def value_load(j):
        return pltpu.make_async_copy(
            wv_hbm.at[0, :, chunk_part(j)], wv.at[:, chunk_part(j)], wv_sem.at[j]
        )

    loads = [
        pltpu.make_async_copy(source.at[0], target, load_sem.at[i])
        for i, (source, target) in enumerate(((wq_hbm, wq), (wk_hbm, wk), (wo_hbm, wo)))
    ]

    barrier = pltpu.get_barrier_semaphore()
    for step in range(1, sections):
        pl.semaphore_signal(
            barrier,
            inc=1,
            device_id={"section": lax.rem(me + step, sections)},
            device_id_type=MESH,
        )

    @pl.when(is_first)
    def _():
        input_load(0).start()

    for j in range(chunks):
        value_load(j).start()
    for load in loads:
        load.start()

    @pl.when(is_first)
    def _():
        for i in range(1, micro):
            input_load(i).start()

    pl.semaphore_wait(barrier, sections - 1)

    onward = jnp.minimum(me + 1, last)

    def h_copy(i):
        return pltpu.make_async_remote_copy(
            src_ref=h_out.at[i],
            dst_ref=h_in.at[i],
            send_sem=hs_sem.at[i],
            recv_sem=hr_sem.at[i],
            device_id={"section": onward},
            device_id_type=MESH,
        )

    def v_copy(i, j):
        return pltpu.make_async_remote_copy(
            src_ref=v_buf.at[i, :, chunk_part(j)],
            dst_ref=v_buf.at[i, :, chunk_part(j)],
            send_sem=vs_sem.at[i, j],
            recv_sem=vr_sem.at[i, j],
            device_id={"section": onward},
            device_id_type=MESH,
        )

    def out_copy(i):
        return pltpu.make_async_remote_copy(
            src_ref=h_out.at[i],
            dst_ref=out_ref.at[i % share],
            send_sem=os_sem.at[i],
            recv_sem=or_sem.at[i],
            device_id={"section": i // share},
            device_id_type=MESH,
        )

    row_index = lax.broadcasted_iota(jnp.int32, (rows, rows), 0)
    column_index = lax.broadcasted_iota(jnp.int32, (rows, rows), 1)
    causal = row_index >= column_index

    def fill_probabilities(normed, arrived):
        arrived(0)
        queries = project(normed, wq[...])
        for n in range(HEADS):
            q_buf[:, head_part(n)] = norm_rows(queries[:, head_part(n)]).astype(bf16)
        arrived(1)
        key_rows = project(normed, wk[...])
        for n in range(HEADS):
            k_buf[:, head_part(n)] = norm_rows(key_rows[:, head_part(n)]).astype(bf16)
        for n in range(HEADS):
            scores = (
                lax.dot_general(
                    q_buf[:, head_part(n)],
                    k_buf[:, head_part(n)],
                    (((1,), (1,)), ((), ())),
                    preferred_element_type=f32,
                )
                * score_scale
            )
            weights = jnp.where(causal, jnp.exp(scores), 0.0)
            p_buf[n] = (weights / jnp.sum(weights, axis=-1, keepdims=True)).astype(bf16)

    @pl.when(is_first)
    def _():
        def one(i, carry):
            input_load(i).wait()
            normed = norm_rows(h_in[i].astype(f32)).astype(bf16)
            for j in range(chunks):

                @pl.when(i == 0)
                def _():
                    value_load(j).wait()

                v_buf[i, :, chunk_part(j)] = project(normed, wv[:, chunk_part(j)]).astype(bf16)
                if sections > 1:

                    @pl.when(i == 0)
                    def _():
                        v_copy(i, j).start()

            def arrived(which):
                @pl.when(i == 0)
                def _():
                    loads[which].wait()

            fill_probabilities(normed, arrived)
            for n in range(HEADS):
                att_buf[:, head_part(n)] = project(p_buf[n], v_buf[i, :, head_part(n)]).astype(bf16)
            arrived(2)
            result = (h_in[i].astype(f32) + project(att_buf[...], wo[...])).astype(bf16)
            if sections > 1:
                h_out[i] = result
                h_copy(i).start()

                @pl.when(i > 0)
                def _():
                    for j in range(chunks):
                        v_copy(i, j).start()

            else:
                out_ref[i] = result
            return carry

        over_sequences(one)

    if sections > 1:

        @pl.when(jnp.logical_not(is_first))
        def _():
            for j in range(chunks):
                value_load(j).wait()
            for load in loads:
                load.wait()
            mixing = mixing_ref[0]

            def one(i, carry):
                h_copy(i).wait_recv()
                normed = norm_rows(h_in[i].astype(f32)).astype(bf16)
                fill_probabilities(normed, lambda which: None)
                val_buf[...] = mixing * project(normed, wv[...])
                for j in range(chunks):
                    v_copy(i, j).wait_recv()
                    if sections > 2:

                        @pl.when(jnp.logical_not(is_last))
                        def _():
                            v_copy(i, j).start()

                    used = (
                        val_buf[:, chunk_part(j)]
                        + (1.0 - mixing) * v_buf[i, :, chunk_part(j)].astype(f32)
                    ).astype(bf16)
                    for n in range(2):
                        att_buf[:, head_part(2 * j + n)] = project(
                            p_buf[2 * j + n], used[:, head_part(n)]
                        ).astype(bf16)
                    term = project(att_buf[:, chunk_part(j)], wo[chunk_part(j), :])
                    if j == 0:
                        acc_buf[...] = term
                    elif j < chunks - 1:
                        acc_buf[...] += term
                result = (h_in[i].astype(f32) + (acc_buf[...] + term)).astype(bf16)
                mine = jnp.logical_and(is_last, i // share == last)

                @pl.when(mine)
                def _():
                    out_ref[i % share] = result

                @pl.when(jnp.logical_not(mine))
                def _():
                    h_out[i] = result

                    @pl.when(is_last)
                    def _():
                        out_copy(i).start()

                    if sections > 2:

                        @pl.when(jnp.logical_not(is_last))
                        def _():
                            h_copy(i).start()

                return carry

            over_sequences(one)

    @pl.when(jnp.logical_not(is_last))
    def _():
        for i in range(micro):
            for j in range(chunks):
                v_copy(i, j).wait_send()
            h_copy(i).wait_send()

    for i in range(micro):
        if i // share != last:

            @pl.when(is_last)
            def _():
                out_copy(i).wait_send()

            @pl.when(me == i // share)
            def _():
                out_copy(i).wait_recv()


def body(inputs, w_query, w_key, w_value, w_out, mixing):
    sections = lax.axis_size("section")
    micro, rows, width = inputs.shape
    features = w_value.shape[2]
    share = micro // sections
    bf16 = jnp.bfloat16
    anywhere = pl.BlockSpec(memory_space=pltpu.HBM)
    dma = pltpu.SemaphoreType.DMA
    return pl.pallas_call(
        functools.partial(kernel, sections),
        out_shape=pltpu.VMEM((share, rows, width), bf16),
        in_specs=[anywhere] * 5 + [pl.BlockSpec(memory_space=pltpu.SMEM)],
        out_specs=pl.BlockSpec(memory_space=pltpu.VMEM),
        scratch_shapes=[
            pltpu.VMEM((width, features), bf16),
            pltpu.VMEM((width, features), bf16),
            pltpu.VMEM((width, features), bf16),
            pltpu.VMEM((features, width), bf16),
            pltpu.VMEM((micro, rows, width), bf16),
            pltpu.VMEM((micro, rows, width), bf16),
            pltpu.VMEM((micro, rows, features), bf16),
            pltpu.VMEM((rows, features), bf16),
            pltpu.VMEM((rows, features), bf16),
            pltpu.VMEM((rows, features), jnp.float32),
            pltpu.VMEM((HEADS, rows, rows), bf16),
            pltpu.VMEM((rows, features), bf16),
            pltpu.VMEM((rows, width), jnp.float32),
            dma((micro,)),
            dma((HEADS // 2,)),
            dma((3,)),
            dma((micro,)),
            dma((micro,)),
            dma((micro, HEADS // 2)),
            dma((micro, HEADS // 2)),
            dma((micro,)),
            dma((micro,)),
        ],
        compiler_params=pltpu.CompilerParams(
            collective_id=0, has_side_effects=True, vmem_limit_bytes=62 * 1024 * 1024
        ),
        name="sections",
    )(inputs, w_query, w_key, w_value, w_out, mixing)


def solution(mesh):
    in_specs = (
        P("dp", None, None),
        P("section", None, None),
        P("section", None, None),
        P("section", None, None),
        P("section", None, None),
        P("section"),
    )
    out_specs = P(("dp", "section"), None, None)
    return jax.shard_map(body, mesh=mesh, in_specs=in_specs, out_specs=out_specs, check_vma=False)
```
